32 devices in a mesh: lat: 8 (over y, x, core), lon: 4 (over z).
Axes of the slice: x: 2, y: 2, z: 4, core: 2. Of those that a mesh axis runs over, the one named last changes fastest.
Arguments:
- right_side: float32 [256, 4096], P('lat', 'lon'), may hold values from -6 to 6
- coefficients: float32 [4, 256, 4096], P(None, 'lat', 'lon'), may hold values from 0.2 to 1.2
- extra: float32 [256, 4096], P('lat', 'lon'), may hold values from 0.05 to 1
- land_mask: int32 [256, 4096], P('lat', 'lon'), may hold values 0 or 1
Outputs:
- solution_field: float32 [256, 4096], P('lat', 'lon')
- residual: float32 [256, 4096], P('lat', 'lon')
- norms: float32 [3], replicated
The draws below stay inside these ranges and needn't reach their ends.
All inputs are finite; a program needn't handle non-finite values. No bound on the sum of `land_mask` on one device may be relied on, other than what follows from the above.
Results may differ from the reference program's by a relative error of at most 0.00028.
Values sent between devices are 32-bit elements; how exact they have to be, the bound alone decides.
A program may use at most 64 MiB of HBM per device.

```python
import math
import jax
import jax.numpy as jnp

DEG = 4
ITERS = 3
NY = 256
NX = 4096


def touch_ends(array, stream_key, least, largest):
    extent = array.shape
    place = [jax.random.randint(jax.random.fold_in(stream_key, axis), (), 0, extent[axis]) for axis in range(len(extent))]
    array = array.at[tuple(place)].set(least)
    longest = extent.index(max(extent))
    place[longest] = (place[longest] + 1) % extent[longest]
    return array.at[tuple(place)].set(largest)


def steps_of(own_key, dims, cuts, least, top_value):
    factor_of, own = 1.0, jax.random.fold_in(own_key, 6)
    for dim, parts in cuts:
        draws = jnp.exp(jax.random.uniform(jax.random.fold_in(own, dim), (parts,), jnp.float32, least / len(cuts), top_value / len(cuts)))
        factor_of = factor_of * jnp.repeat(draws, dims[dim] // parts).reshape([-1 if axis == dim else 1 for axis in range(len(dims))])
    return factor_of


def noise(own_key, dims, deviation, reach, split=(), kind=jnp.bfloat16):
    array = deviation * jax.random.normal(own_key, dims, jnp.float32)
    if split:
        array = array * steps_of(own_key, dims, split, -0.22, 0.18)
    return jnp.clip(array, -reach, reach).astype(kind)


def setup_inputs(seed: int = 0) -> dict:
    splits = jax.random.split(jax.random.key(seed), 5)
    right_side = noise(splits[0], (NY, NX), 1.0, 6.0, ((0, 8), (1, 4)), jnp.float32)
    coefficients = jnp.clip(0.2 + 1 * jax.random.uniform(splits[1], (4, NY, NX), jnp.float32) ** steps_of(splits[1], (4, NY, NX), ((1, 8), (2, 4)), -0.2, 0.2), 0.2, 1.2)
    extra = jnp.clip(jnp.exp(math.log(1.0) - 2.9957323 * jax.random.uniform(splits[2], (NY, NX), jnp.float32) ** steps_of(splits[2], (NY, NX), ((0, 8), (1, 4)), -0.2, 0.2)), 0.05, 1.0)
    land_mask = touch_ends((jax.random.randint(splits[3], (NY, NX), 0, 5) < 4).astype(jnp.int32), jax.random.fold_in(splits[3], 1), 0, 1)
    return {"right_side": right_side, "coefficients": coefficients, "extra": extra, "land_mask": land_mask}


LOW_EIG = 0.25
HIGH_EIG = 20.5


def east(a):
    return jnp.roll(a, -1, axis=1)


def west(a):
    return jnp.roll(a, 1, axis=1)


def north(a):
    return jnp.roll(a, -1, axis=0)


def south(a):
    return jnp.roll(a, 1, axis=0)


def operate(v, diag, le, ln, lne, lnw):
    out = diag * v - le * east(v) - west(le) * west(v)
    out = out - ln * north(v) - south(ln) * south(v)
    out = out - lne * north(east(v)) - south(west(lne)) * south(west(v))
    out = out - lnw * north(west(v)) - south(east(lnw)) * south(east(v))
    return out


def chebyshev(r, mat):
    theta = (HIGH_EIG + LOW_EIG) / 2.0
    delta = (HIGH_EIG - LOW_EIG) / 2.0
    sigma = theta / delta
    rho = 1.0 / sigma
    step = r / theta
    z = step
    for level in range(DEG - 1):
        q = r - mat(z)
        rho_new = 1.0 / (2.0 * sigma - rho)
        step = (rho_new * rho) * step + (2.0 * rho_new / delta) * q
        z = z + step
        rho = rho_new
    return z


def reference(right_side, coefficients, extra, land_mask):
    m = land_mask.astype(jnp.float32)
    rows = jnp.arange(NY, dtype=jnp.int32)
    keep = (rows != NY - 1).astype(jnp.float32)[:, None]
    le = coefficients[0] * m * east(m)
    ln = coefficients[1] * m * north(m) * keep
    lne = coefficients[2] * m * north(east(m)) * keep
    lnw = coefficients[3] * m * north(west(m)) * keep
    diag = extra + le + west(le) + ln + south(ln) + lne + south(west(lne)) + lnw + south(east(lnw))

    def mat(v):
        return operate(v, diag, le, ln, lne, lnw)

    r = m * right_side
    x = jnp.zeros_like(r)
    u = chebyshev(r, mat)
    w = mat(u)
    gamma = jnp.sum(r * u)
    dlt = jnp.sum(w * u)
    norms = [jnp.sum(r * r)]
    alpha = gamma / dlt
    p = u
    s = w
    beta = jnp.float32(0.0)
    for k in range(ITERS):
        if k > 0:
            p = u + beta * p
            s = w + beta * s
        x = x + alpha * p
        r = r - alpha * s
        if k < ITERS - 1:
            u = chebyshev(r, mat)
            w = mat(u)
            gamma_new = jnp.sum(r * u)
            dlt = jnp.sum(w * u)
            norms.append(jnp.sum(r * r))
            beta = gamma_new / gamma
            alpha = gamma_new / (dlt - beta * gamma_new / alpha)
            gamma = gamma_new
    return x, r, jnp.stack(norms).astype(jnp.float32)
```

```python
import functools

import jax
import jax.numpy as jnp
from jax import lax
from jax.experimental import pallas as pl
from jax.experimental.pallas import tpu as pltpu
from jax.sharding import PartitionSpec as P

DEG = 4
ITERS = 3
LOW_EIG = 0.25
HIGH_EIG = 20.5
SHIFT = 0.8
LANES = 128
HALO = 16
MESH = pl.DeviceIdType.MESH
DIRS = [(a, b) for a in (-1, 0, 1) for b in (-1, 0, 1) if (a, b) != (0, 0)]


def level_factors():
    theta = (HIGH_EIG + LOW_EIG) / 2.0
    delta = (HIGH_EIG - LOW_EIG) / 2.0
    sigma = theta / delta
    rho = 1.0 / sigma
    out = []
    for _ in range(DEG - 1):
        rho_new = 1.0 / (2.0 * sigma - rho)
        out.append((rho_new * rho, 2.0 * rho_new / delta))
        rho = rho_new
    return theta, out


def scalars(h, g):
    c = SHIFT
    ht = [h[k + 1] + c * h[k] for k in range(len(h) - 1)]

    def form(a, t):
        total = None
        for k in range(2 * len(a) - 1):
            pairs = None
            for i in range(len(a)):
                j = k - i
                if 0 <= j < len(a) and i <= j:
                    term = a[i] * a[j]
                    if i != j:
                        term = term + term
                    pairs = term if pairs is None else pairs + term
            pairs = pairs * t[k]
            total = pairs if total is None else total + pairs
        return total

    one = jnp.ones_like(h[0])
    zero = jnp.zeros_like(h[0])
    a = [one]
    b = [one]
    gamma = h[0]
    norms = [g[0]]
    alpha = gamma / ht[0]
    x = [zero] * ITERS
    beta = zero
    for k in range(ITERS):
        if k > 0:
            b = [a[i] + (beta * b[i] if i < len(b) else 0.0) for i in range(len(a))]
        for i in range(len(b)):
            x[i] = x[i] + alpha * b[i]
        tb = [
            (b[i - 1] if i > 0 else zero) + (c * b[i] if i < len(b) else zero)
            for i in range(len(b) + 1)
        ]
        a = [(a[i] if i < len(a) else zero) - alpha * tb[i] for i in range(len(tb))]
        if k < ITERS - 1:
            gamma_new = form(a, h)
            dlt = form(a, ht)
            norms.append(form(a, g))
            beta = gamma_new / gamma
            alpha = gamma_new / (dlt - beta * gamma_new / alpha)
            gamma = gamma_new
    return x, a, norms


def kernel(
    nlat, nlon, rhs_in, coef_in, extra_in, mask_in, x_out, r_out, n_out,
    B, C, E, M, K, V, U, S, Z, G, GL, GZ, T2,
    loc_sem, snd, rcv, lat_s, lat_r, lon_s, lon_r,
):
    rows, cols = rhs_in.shape
    R = rows + 2 * HALO
    W = cols + 2 * LANES
    NC = W // LANES
    ilat = lax.axis_index("lat")
    ilon = lax.axis_index("lon")

    mid = (pl.ds(HALO, rows), pl.ds(LANES, cols))
    local = [
        pltpu.make_async_copy(coef_in, C.at[:, mid[0], mid[1]], loc_sem.at[0]),
        pltpu.make_async_copy(mask_in, M.at[mid[0], mid[1]], loc_sem.at[1]),
        pltpu.make_async_copy(extra_in, E.at[mid[0], mid[1]], loc_sem.at[2]),
        pltpu.make_async_copy(rhs_in, B.at[mid[0], mid[1]], loc_sem.at[3]),
    ]
    for cp in local:
        cp.start()

    def lat_at(d):
        return lax.rem(ilat + d + nlat, nlat)

    def lon_at(d):
        return lax.rem(ilon + d + nlon, nlon)

    barrier = pltpu.get_barrier_semaphore()
    count = 0
    for d in range(1, nlat):
        pl.semaphore_signal(barrier, inc=1, device_id={"lat": lat_at(d)}, device_id_type=MESH)
        count += 1
    for d in range(1, nlon):
        pl.semaphore_signal(barrier, inc=1, device_id={"lon": lon_at(d)}, device_id_type=MESH)
        count += 1
    for a, b in DIRS:
        if a and b:
            pl.semaphore_signal(
                barrier, inc=1, device_id={"lat": lat_at(a), "lon": lon_at(b)}, device_id_type=MESH
            )
            count += 1
    pl.semaphore_wait(barrier, count)

    def region(d, size, pad, width):
        if d == 0:
            return pad, pad, size
        if d > 0:
            return pad + size - width, 0, width
        return pad, pad + size, width

    sends = []
    for f in range(4):
        local[f].wait()
        for i, (a, b) in enumerate(DIRS):
            rs, rd, rn = region(a, rows, HALO, HALO)
            cs, cd, cn = region(b, cols, LANES, LANES)
            ref = (C, M, E, B)[f]
            lead = (slice(None),) if f == 0 else ()
            where = {}
            if a:
                where["lat"] = lat_at(a)
            if b:
                where["lon"] = lon_at(b)
            cp = pltpu.make_async_remote_copy(
                src_ref=ref.at[(*lead, pl.ds(rs, rn), pl.ds(cs, cn))],
                dst_ref=ref.at[(*lead, pl.ds(rd, rn), pl.ds(cd, cn))],
                send_sem=snd.at[i, f],
                recv_sem=rcv.at[i, f],
                device_id=where,
                device_id_type=MESH,
            )
            cp.start()
            sends.append(cp)
    for cp in sends:
        cp.wait_recv()

    lane = lax.broadcasted_iota(jnp.int32, (R, LANES), 1)
    first = lane == 0
    last = lane == LANES - 1

    def cs_of(j):
        return pl.ds(pl.multiple_of(j * LANES, LANES), LANES)

    def neighbours(j):
        return lax.rem(j + NC - 1, NC), lax.rem(j + 1, NC)

    def east(c, e):
        return jnp.where(last, pltpu.roll(e, LANES - 1, 1), pltpu.roll(c, LANES - 1, 1))

    def west(c, w):
        return jnp.where(first, pltpu.roll(w, 1, 1), pltpu.roll(c, 1, 1))

    def north(a):
        return pltpu.roll(a, R - 1, 0)

    def south(a):
        return pltpu.roll(a, 1, 0)

    grow = lax.broadcasted_iota(jnp.int32, (R, LANES), 0) + (ilat * rows - HALO)
    keep = jnp.where((grow == nlat * rows - 1) | (grow == -1), 0.0, 1.0).astype(jnp.float32)

    @pl.loop(0, NC)
    def _(j):
        wj, ej = neighbours(j)
        m = M[:, cs_of(j)].astype(jnp.float32)
        me = east(m, M[:, cs_of(ej)].astype(jnp.float32))
        mw = west(m, M[:, cs_of(wj)].astype(jnp.float32))
        mk = m * keep
        K[1, :, cs_of(j)] = C[0, :, cs_of(j)] * m * me
        K[6, :, cs_of(j)] = C[1, :, cs_of(j)] * mk * north(m)
        K[9, :, cs_of(j)] = C[2, :, cs_of(j)] * mk * north(me)
        K[10, :, cs_of(j)] = C[3, :, cs_of(j)] * mk * north(mw)
        V[0, :, cs_of(j)] = B[:, cs_of(j)] * m

    @pl.loop(0, NC)
    def _(j):
        wj, ej = neighbours(j)
        le = K[1, :, cs_of(j)]
        wle = west(le, K[1, :, cs_of(wj)])
        ln = K[6, :, cs_of(j)]
        sln = south(ln)
        lne = K[9, :, cs_of(j)]
        wlne = west(lne, K[9, :, cs_of(wj)])
        lnw = K[10, :, cs_of(j)]
        elnw = east(lnw, K[10, :, cs_of(ej)])
        K[2, :, cs_of(j)] = wle
        K[3, :, cs_of(j)] = sln
        K[4, :, cs_of(j)] = south(lne)
        K[5, :, cs_of(j)] = south(lnw)
        K[7, :, cs_of(j)] = wlne
        K[8, :, cs_of(j)] = elnw
        d = E[:, cs_of(j)] + le + wle + ln + sln
        K[0, :, cs_of(j)] = d + lne + south(wlne) + lnw + south(elnw)

    def image(read, j):
        wj, ej = neighbours(j)
        v = read(j)
        ve = east(v, read(ej))
        vw = west(v, read(wj))

        def k(n):
            return K[n, :, cs_of(j)]

        p = k(3) * v + k(4) * ve + k(5) * vw
        q = k(6) * v + k(7) * vw + k(8) * ve
        out = k(0) * v - k(1) * ve - k(2) * vw - north(p) - south(q)
        return v, out

    theta, factors = level_factors()

    @pl.loop(0, ITERS)
    def _(it):
        @pl.loop(0, NC)
        def _(j):
            v, av = image(lambda t: V[it, :, cs_of(t)], j)
            z = v * (1.0 / theta)
            step = factors[0][0] * z + factors[0][1] * (v - av * (1.0 / theta))
            S[:, cs_of(j)] = step
            Z[0, :, cs_of(j)] = z + step

        for level in range(1, DEG - 1):
            src = (level - 1) % 2

            @pl.loop(0, NC)
            def _(j):
                z, az = image(lambda t: Z[src, :, cs_of(t)], j)
                qq = V[it, :, cs_of(j)] - az
                step = factors[level][0] * S[:, cs_of(j)] + factors[level][1] * qq
                if level < DEG - 2:
                    S[:, cs_of(j)] = step
                    Z[1 - src, :, cs_of(j)] = z + step
                else:
                    U[it, :, cs_of(j)] = z + step

        @pl.loop(0, NC)
        def _(j):
            _, au = image(lambda t: U[it, :, cs_of(t)], j)
            V[it + 1, :, cs_of(j)] = au - SHIFT * V[it, :, cs_of(j)]

    hpairs = [((k + 1) // 2, k // 2) for k in range(2 * ITERS)]
    gpairs = [(k // 2, (k + 1) // 2) for k in range(2 * ITERS - 1)]

    def own(ref, n, j):
        return ref[n, pl.ds(HALO, rows), cs_of(j)]

    def fold(a):
        return jnp.sum(a.reshape(rows // 8, 8, LANES), axis=0)

    def add(j, acc):
        v = [own(V, n, j) for n in range(ITERS + 1)]
        u = [own(U, n, j) for n in range(ITERS)]
        new = [fold(v[a] * u[b]) for a, b in hpairs] + [fold(v[a] * v[b]) for a, b in gpairs]
        return tuple(p + q for p, q in zip(acc, new))

    nsum = len(hpairs) + len(gpairs)
    acc = lax.fori_loop(
        1, NC - 1, add, tuple(jnp.zeros((8, LANES), jnp.float32) for _ in range(nsum))
    )
    T2[...] = jnp.zeros_like(T2)
    for n, a in enumerate(acc):
        T2[n : n + 1, :] = jnp.sum(a, axis=0, keepdims=True)
    lo = T2[0:8, :]
    hi = T2[8:16, :]
    lo = lo + pltpu.roll(lo, LANES // 2, 1)
    hi = hi + pltpu.roll(hi, LANES // 2, 1)
    half = lax.broadcasted_iota(jnp.int32, (8, LANES), 1) < LANES // 2
    part = jnp.where(half, lo, hi)

    def exchange(part, slot, buf, axis, count, me, at, ssem, rsem):
        G[slot] = part
        buf[me] = part
        cps = []
        for d in range(1, count):
            cp = pltpu.make_async_remote_copy(
                src_ref=G.at[slot],
                dst_ref=buf.at[me],
                send_sem=ssem.at[d],
                recv_sem=rsem.at[d],
                device_id={axis: at(d)},
                device_id_type=MESH,
            )
            cp.start()
            cps.append(cp)
        for cp in cps:
            cp.wait_recv()
        total = buf[0]
        for n in range(1, count):
            total = total + buf[n]
        return total, cps

    total, c1 = exchange(part, 0, GL, "lat", nlat, ilat, lat_at, lat_s, lat_r)
    total, c2 = exchange(total, 1, GZ, "lon", nlon, ilon, lon_at, lon_s, lon_r)

    for n, t in enumerate((jnp.where(half, total, 0.0), jnp.where(half, 0.0, total))):
        s = jnp.sum(t, axis=1, keepdims=True)
        T2[8 * n : 8 * n + 8, :] = jnp.broadcast_to(s, (8, LANES))
    sums = [T2[n : n + 1, :] for n in range(nsum)]
    xs, rs, norms = scalars(sums[: len(hpairs)], sums[len(hpairs) :])

    @pl.loop(0, NC - 2)
    def _(j):
        x = xs[0] * own(U, 0, j + 1)
        for n in range(1, ITERS):
            x = x + xs[n] * own(U, n, j + 1)
        x_out[:, cs_of(j)] = x
        r = rs[0] * own(V, 0, j + 1)
        for n in range(1, ITERS + 1):
            r = r + rs[n] * own(V, n, j + 1)
        r_out[:, cs_of(j)] = r

    for n in range(ITERS):
        n_out[n] = norms[n][0, 0]
    for cp in sends + c1 + c2:
        cp.wait_send()


def solution(mesh):
    nlat = mesh.shape["lat"]
    nlon = mesh.shape["lon"]

    def body(right_side, coefficients, extra, land_mask):
        rows, cols = right_side.shape
        R, W = rows + 2 * HALO, cols + 2 * LANES
        f32 = jnp.float32
        return pl.pallas_call(
            functools.partial(kernel, nlat, nlon),
            out_shape=(
                jax.ShapeDtypeStruct((rows, cols), f32),
                jax.ShapeDtypeStruct((rows, cols), f32),
                jax.ShapeDtypeStruct((ITERS,), f32),
            ),
            in_specs=[pl.BlockSpec(memory_space=pl.ANY)] * 4,
            out_specs=(
                pl.BlockSpec(memory_space=pltpu.VMEM),
                pl.BlockSpec(memory_space=pltpu.VMEM),
                pl.BlockSpec(memory_space=pltpu.SMEM),
            ),
            scratch_shapes=[
                pltpu.VMEM((R, W), f32),
                pltpu.VMEM((4, R, W), f32),
                pltpu.VMEM((R, W), f32),
                pltpu.VMEM((R, W), jnp.int32),
                pltpu.VMEM((11, R, W), f32),
                pltpu.VMEM((ITERS + 1, R, W), f32),
                pltpu.VMEM((ITERS, R, W), f32),
                pltpu.VMEM((R, W), f32),
                pltpu.VMEM((2, R, W), f32),
                pltpu.VMEM((2, 8, LANES), f32),
                pltpu.VMEM((nlat, 8, LANES), f32),
                pltpu.VMEM((nlon, 8, LANES), f32),
                pltpu.VMEM((16, LANES), f32),
                pltpu.SemaphoreType.DMA((4,)),
                pltpu.SemaphoreType.DMA((8, 4)),
                pltpu.SemaphoreType.DMA((8, 4)),
                pltpu.SemaphoreType.DMA((nlat,)),
                pltpu.SemaphoreType.DMA((nlat,)),
                pltpu.SemaphoreType.DMA((nlon,)),
                pltpu.SemaphoreType.DMA((nlon,)),
            ],
            compiler_params=pltpu.CompilerParams(
                collective_id=0, has_side_effects=True, vmem_limit_bytes=32 * 1024 * 1024
            ),
        )(right_side, coefficients, extra, land_mask)

    return jax.shard_map(
        body,
        mesh=mesh,
        in_specs=(P("lat", "lon"), P(None, "lat", "lon"), P("lat", "lon"), P("lat", "lon")),
        out_specs=(P("lat", "lon"), P("lat", "lon"), P()),
        check_vma=False,
    )
```

```python
import functools

import jax
import jax.numpy as jnp
from jax import lax
from jax.experimental import pallas as pl
from jax.experimental.pallas import tpu as pltpu
from jax.sharding import PartitionSpec as P

DEG = 4
ITERS = 3
LOW_EIG = 0.25
HIGH_EIG = 20.5
SHIFT = 0.8
LANES = 128
HALO = 16
STRIP = 16
FIELDS = 7
PAIRS = (FIELDS + 1) // 2
MESH = pl.DeviceIdType.MESH
DIRS = [(a, b) for a in (-1, 0, 1) for b in (-1, 0, 1) if (a, b) != (0, 0)]


def level_factors():
    theta = (HIGH_EIG + LOW_EIG) / 2.0
    delta = (HIGH_EIG - LOW_EIG) / 2.0
    sigma = theta / delta
    rho = 1.0 / sigma
    out = []
    for _ in range(DEG - 1):
        rho_new = 1.0 / (2.0 * sigma - rho)
        out.append((rho_new * rho, 2.0 * rho_new / delta))
        rho = rho_new
    return theta, out


def scalars(h, g):
    c = SHIFT
    ht = [h[k + 1] + c * h[k] for k in range(len(h) - 1)]

    def form(a, t):
        total = None
        for k in range(2 * len(a) - 1):
            pairs = None
            for i in range(len(a)):
                j = k - i
                if 0 <= j < len(a) and i <= j:
                    term = a[i] * a[j]
                    if i != j:
                        term = term + term
                    pairs = term if pairs is None else pairs + term
            pairs = pairs * t[k]
            total = pairs if total is None else total + pairs
        return total

    one = jnp.ones_like(h[0])
    zero = jnp.zeros_like(h[0])
    a = [one]
    b = [one]
    gamma = h[0]
    norms = [g[0]]
    alpha = gamma / ht[0]
    x = [zero] * ITERS
    beta = zero
    for k in range(ITERS):
        if k > 0:
            b = [a[i] + (beta * b[i] if i < len(b) else 0.0) for i in range(len(a))]
        for i in range(len(b)):
            x[i] = x[i] + alpha * b[i]
        tb = [
            (b[i - 1] if i > 0 else zero) + (c * b[i] if i < len(b) else zero)
            for i in range(len(b) + 1)
        ]
        a = [(a[i] if i < len(a) else zero) - alpha * tb[i] for i in range(len(tb))]
        if k < ITERS - 1:
            gamma_new = form(a, h)
            dlt = form(a, ht)
            norms.append(form(a, g))
            beta = gamma_new / gamma
            alpha = gamma_new / (dlt - beta * gamma_new / alpha)
            gamma = gamma_new
    return x, a, norms


def kernel(
    nlat, nlon, rhs_in, coef_in, extra_in, mask_in, x_out, r_out, n_out,
    B, C, E, M, K, V, U, VC, UC, S, Z, SP, RP, SR, RR, G, GL, GZ, T2,
    loc_sem, snd, rcv, lat_s, lat_r, lon_s, lon_r,
):
    rows, cols = rhs_in.shape
    R = rows + 2 * HALO
    W = cols + 2 * LANES
    NC = W // LANES
    ilat = lax.axis_index("lat")
    ilon = lax.axis_index("lon")

    def cs_of(j):
        return slice(j * LANES, (j + 1) * LANES)

    mid = (pl.ds(HALO, rows), pl.ds(LANES, cols))
    local = [
        pltpu.make_async_copy(coef_in, C.at[:, mid[0], mid[1]], loc_sem.at[0]),
        pltpu.make_async_copy(mask_in, M.at[mid[0], mid[1]], loc_sem.at[1]),
        pltpu.make_async_copy(extra_in, E.at[mid[0], mid[1]], loc_sem.at[2]),
        pltpu.make_async_copy(rhs_in, B.at[mid[0], mid[1]], loc_sem.at[3]),
    ]
    for cp in local:
        cp.start()

    def lat_at(d):
        return lax.rem(ilat + d + nlat, nlat)

    def lon_at(d):
        return lax.rem(ilon + d + nlon, nlon)

    barrier = pltpu.get_barrier_semaphore()
    count = 0
    for d in range(1, nlat):
        pl.semaphore_signal(barrier, inc=1, device_id={"lat": lat_at(d)}, device_id_type=MESH)
        count += 1
    for d in range(1, nlon):
        pl.semaphore_signal(barrier, inc=1, device_id={"lon": lon_at(d)}, device_id_type=MESH)
        count += 1
    for a, b in DIRS:
        if a and b:
            pl.semaphore_signal(
                barrier, inc=1, device_id={"lat": lat_at(a), "lon": lon_at(b)}, device_id_type=MESH
            )
            count += 1
    for cp in local:
        cp.wait()

    def field(f, rws, cls):
        if f < 4:
            return C[f, rws, cls]
        if f == 4:
            return E[rws, cls]
        if f == 5:
            return B[rws, cls]
        return M[rws, cls].astype(jnp.float32)

    def put(f, rws, cls, value):
        if f < 4:
            C[f, rws, cls] = value
        elif f == 4:
            E[rws, cls] = value
        elif f == 5:
            B[rws, cls] = value
        else:
            M[rws, cls] = value.astype(jnp.int32)

    own_rows = slice(HALO, HALO + rows)
    slot = lax.broadcasted_iota(jnp.int32, (rows, LANES), 1) // STRIP
    for side, chunk in ((0, 1), (1, NC - 2)):
        strip = jnp.zeros((rows, LANES), jnp.float32)
        for f in range(FIELDS):
            turn = (STRIP * f + side * STRIP) % LANES
            a = field(f, own_rows, cs_of(chunk))
            a = pltpu.roll(a, turn, 1) if turn else a
            strip = jnp.where(slot == f, a, strip)
        SP[side] = strip
    upper = lax.broadcasted_iota(jnp.int32, (8, cols), 0) >= 4
    inner = slice(LANES, LANES + cols)
    near = (slice(HALO + 8, HALO + 16), slice(HALO + rows - 16, HALO + rows - 8))
    for side in (0, 1):
        for t in range(PAIRS):
            a = field(2 * t, near[side], inner)
            if 2 * t + 1 < FIELDS:
                b = pltpu.roll(field(2 * t + 1, near[side], inner), 4, 0)
                a = jnp.where(upper, a, b) if side else jnp.where(upper, b, a)
            SR[side, t] = a
    pl.semaphore_wait(barrier, count)

    sends = []

    def send(src, dst, a, b):
        i = len(sends)
        where = {}
        if a:
            where["lat"] = lat_at(a)
        if b:
            where["lon"] = lon_at(b)
        cp = pltpu.make_async_remote_copy(
            src_ref=src, dst_ref=dst, send_sem=snd.at[i], recv_sem=rcv.at[i],
            device_id=where, device_id_type=MESH,
        )
        cp.start()
        sends.append(cp)

    for a in (-1, 1):
        side = (a + 1) // 2
        src = pl.ds(HALO, 8) if a < 0 else pl.ds(HALO + rows - 8, 8)
        dst = pl.ds(HALO + rows, 8) if a < 0 else pl.ds(HALO - 8, 8)
        wide = pl.ds(LANES, cols)
        send(C.at[:, src, wide], C.at[:, dst, wide], a, 0)
        for ref in (E, B, M):
            send(ref.at[src, wide], ref.at[dst, wide], a, 0)
        send(SR.at[side], RR.at[side], a, 0)
    for b in (-1, 1):
        side = (b + 1) // 2
        send(SP.at[side], RP.at[side, pl.ds(HALO, rows)], 0, b)
        for a in (-1, 1):
            src = pl.ds(0, HALO) if a < 0 else pl.ds(rows - HALO, HALO)
            dst = pl.ds(HALO + rows, HALO) if a < 0 else pl.ds(0, HALO)
            send(SP.at[side, src], RP.at[side, dst], a, b)
    for cp in sends:
        cp.wait_recv()

    every = slice(0, R)
    for side, chunk in ((0, NC - 1), (1, 0)):
        strip = RP[side]
        for f in range(FIELDS):
            turn = (-STRIP * f - side * STRIP) % LANES
            put(f, every, cs_of(chunk), pltpu.roll(strip, turn, 1) if turn else strip)
    far = (slice(R - 8, R), slice(0, 8))
    for side in (0, 1):
        for f in range(FIELDS):
            a = RR[side, f // 2]
            put(f, far[side], inner, pltpu.roll(a, 4, 0) if f % 2 else a)

    def shifts(read, n):
        lane = lax.broadcasted_iota(jnp.int32, (n, LANES), 1)
        first = lane == 0
        last = lane == LANES - 1
        memo = {}

        def get(kind, j):
            j = j % NC
            if (kind, j) not in memo:
                if kind == 0:
                    memo[kind, j] = read(j)
                else:
                    memo[kind, j] = pltpu.roll(get(0, j), 1 if kind < 0 else LANES - 1, 1)
            return memo[kind, j]

        def east(j):
            return jnp.where(last, get(1, j + 1), get(1, j))

        def west(j):
            return jnp.where(first, get(-1, j - 1), get(-1, j))

        return (lambda j: get(0, j)), east, west

    def north(a):
        return pltpu.roll(a, a.shape[0] - 1, 0)

    def south(a):
        return pltpu.roll(a, 1, 0)

    grow = lax.broadcasted_iota(jnp.int32, (R, LANES), 0) + (ilat * rows - HALO)
    keep = jnp.where((grow == nlat * rows - 1) | (grow == -1), 0.0, 1.0).astype(jnp.float32)

    mc, mE, mW = shifts(lambda j: M[:, cs_of(j)].astype(jnp.float32), R)
    for j in range(NC):
        m = mc(j)
        me = mE(j)
        mw = mW(j)
        mk = m * keep
        K[1][:, cs_of(j)] = C[0, :, cs_of(j)] * m * me
        K[6][:, cs_of(j)] = C[1, :, cs_of(j)] * mk * north(m)
        K[9][:, cs_of(j)] = C[2, :, cs_of(j)] * mk * north(me)
        K[10][:, cs_of(j)] = C[3, :, cs_of(j)] * mk * north(mw)
        VC[:, cs_of(j)] = B[:, cs_of(j)] * m

    cle, _, wle_of = shifts(lambda j: K[1][:, cs_of(j)], R)
    clne, _, wlne_of = shifts(lambda j: K[9][:, cs_of(j)], R)
    clnw, elnw_of, _ = shifts(lambda j: K[10][:, cs_of(j)], R)
    for j in range(NC):
        le = cle(j)
        wle = wle_of(j)
        ln = K[6][:, cs_of(j)]
        sln = south(ln)
        lne = clne(j)
        wlne = wlne_of(j)
        lnw = clnw(j)
        elnw = elnw_of(j)
        K[2][:, cs_of(j)] = wle
        K[3][:, cs_of(j)] = sln
        K[4][:, cs_of(j)] = south(lne)
        K[5][:, cs_of(j)] = south(lnw)
        K[7][:, cs_of(j)] = wlne
        K[8][:, cs_of(j)] = elnw
        d = E[:, cs_of(j)] + le + wle + ln + sln
        K[0][:, cs_of(j)] = d + lne + south(wlne) + lnw + south(elnw)

    theta, factors = level_factors()

    def apply(ref, rws, finish):
        n = rws.stop - rws.start
        centre, east, west = shifts(lambda j: ref[rws, cs_of(j)], n)
        for j in range(NC):
            v = centre(j)
            ve = east(j)
            vw = west(j)

            def k(i):
                return K[i][rws, cs_of(j)]

            p = k(3) * v + k(4) * ve + k(5) * vw
            q = k(6) * v + k(7) * vw + k(8) * ve
            finish(cs_of(j), v, k(0) * v - k(1) * ve - k(2) * vw - north(p) - south(q))

    mine = slice(HALO, HALO + rows)

    def round_of(it, rws):
        lo = HALO - rws.start

        def level0(cls, v, av):
            z = v * (1.0 / theta)
            step = factors[0][0] * z + factors[0][1] * (v - av * (1.0 / theta))
            S[rws, cls] = step
            Z[0][rws, cls] = z + step

        apply(VC, rws, level0)
        for level in range(1, DEG - 1):
            src = (level - 1) % 2

            def inner_level(cls, z, az):
                qq = VC[rws, cls] - az
                step = factors[level][0] * S[rws, cls] + factors[level][1] * qq
                new = z + step
                if level < DEG - 2:
                    S[rws, cls] = step
                    Z[1 - src][rws, cls] = new
                else:
                    UC[rws, cls] = new
                    U[it, :, cls] = new[lo : lo + rows]

            apply(Z[src], rws, inner_level)

        def last_level(cls, u, au):
            new = au - SHIFT * VC[rws, cls]
            VC[rws, cls] = new
            V[it + 1, :, cls] = new[lo : lo + rows]

        apply(UC, rws, last_level)

    for j in range(1, NC - 1):
        V[0, :, cs_of(j)] = VC[mine, cs_of(j)]
    round_of(0, slice(0, R))

    @pl.loop(1, ITERS)
    def _(it):
        round_of(it, slice(8, R - 8))

    hpairs = [((k + 1) // 2, k // 2) for k in range(2 * ITERS)]
    gpairs = [(k // 2, (k + 1) // 2) for k in range(2 * ITERS - 1)]

    def own(ref, n, j):
        return ref[n, :, cs_of(j)]

    def fold(a):
        return jnp.sum(a.reshape(rows // 8, 8, LANES), axis=0)

    def add(j, acc):
        v = [own(V, n, j) for n in range(ITERS + 1)]
        u = [own(U, n, j) for n in range(ITERS)]
        new = [fold(v[a] * u[b]) for a, b in hpairs] + [fold(v[a] * v[b]) for a, b in gpairs]
        return tuple(p + q for p, q in zip(acc, new))

    nsum = len(hpairs) + len(gpairs)
    acc = tuple(jnp.zeros((8, LANES), jnp.float32) for _ in range(nsum))
    for j in range(1, NC - 1):
        acc = add(j, acc)
    T2[...] = jnp.zeros_like(T2)
    for n, a in enumerate(acc):
        T2[n : n + 1, :] = jnp.sum(a, axis=0, keepdims=True)
    lo = T2[0:8, :]
    hi = T2[8:16, :]
    lo = lo + pltpu.roll(lo, LANES // 2, 1)
    hi = hi + pltpu.roll(hi, LANES // 2, 1)
    half = lax.broadcasted_iota(jnp.int32, (8, LANES), 1) < LANES // 2
    part = jnp.where(half, lo, hi)

    def exchange(part, slot, buf, axis, count, me, at, ssem, rsem):
        G[slot] = part
        buf[me] = part
        cps = []
        for d in range(1, count):
            cp = pltpu.make_async_remote_copy(
                src_ref=G.at[slot],
                dst_ref=buf.at[me],
                send_sem=ssem.at[d],
                recv_sem=rsem.at[d],
                device_id={axis: at(d)},
                device_id_type=MESH,
            )
            cp.start()
            cps.append(cp)
        for cp in cps:
            cp.wait_recv()
        total = buf[0]
        for n in range(1, count):
            total = total + buf[n]
        return total, cps

    total, c1 = exchange(part, 0, GL, "lat", nlat, ilat, lat_at, lat_s, lat_r)
    total, c2 = exchange(total, 1, GZ, "lon", nlon, ilon, lon_at, lon_s, lon_r)

    for n, t in enumerate((jnp.where(half, total, 0.0), jnp.where(half, 0.0, total))):
        s = jnp.sum(t, axis=1, keepdims=True)
        T2[8 * n : 8 * n + 8, :] = jnp.broadcast_to(s, (8, LANES))
    sums = [T2[n : n + 1, :] for n in range(nsum)]
    xs, rs, norms = scalars(sums[: len(hpairs)], sums[len(hpairs) :])

    for j in range(NC - 2):
        x = xs[0] * own(U, 0, j + 1)
        for n in range(1, ITERS):
            x = x + xs[n] * own(U, n, j + 1)
        x_out[:, cs_of(j)] = x
        r = rs[0] * own(V, 0, j + 1)
        for n in range(1, ITERS + 1):
            r = r + rs[n] * own(V, n, j + 1)
        r_out[:, cs_of(j)] = r

    for n in range(ITERS):
        n_out[n] = norms[n][0, 0]
    for cp in sends + c1 + c2:
        cp.wait_send()


def solution(mesh):
    nlat = mesh.shape["lat"]
    nlon = mesh.shape["lon"]

    def body(right_side, coefficients, extra, land_mask):
        rows, cols = right_side.shape
        R, W = rows + 2 * HALO, cols + 2 * LANES
        f32 = jnp.float32
        return pl.pallas_call(
            functools.partial(kernel, nlat, nlon),
            out_shape=(
                jax.ShapeDtypeStruct((rows, cols), f32),
                jax.ShapeDtypeStruct((rows, cols), f32),
                jax.ShapeDtypeStruct((ITERS,), f32),
            ),
            in_specs=[pl.BlockSpec(memory_space=pl.ANY)] * 4,
            out_specs=(
                pl.BlockSpec(memory_space=pltpu.VMEM),
                pl.BlockSpec(memory_space=pltpu.VMEM),
                pl.BlockSpec(memory_space=pltpu.SMEM),
            ),
            scratch_shapes=[
                pltpu.VMEM((R, W), f32),
                pltpu.VMEM((4, R, W), f32),
                pltpu.VMEM((R, W), f32),
                pltpu.VMEM((R, W), jnp.int32),
                [pltpu.VMEM((R, W), f32)] * 11,
                pltpu.VMEM((ITERS + 1, rows, W), f32),
                pltpu.VMEM((ITERS, rows, W), f32),
                pltpu.VMEM((R, W), f32),
                pltpu.VMEM((R, W), f32),
                pltpu.VMEM((R, W), f32),
                [pltpu.VMEM((R, W), f32)] * 2,
                pltpu.VMEM((2, rows, LANES), f32),
                pltpu.VMEM((2, R, LANES), f32),
                pltpu.VMEM((2, PAIRS, 8, cols), f32),
                pltpu.VMEM((2, PAIRS, 8, cols), f32),
                pltpu.VMEM((2, 8, LANES), f32),
                pltpu.VMEM((nlat, 8, LANES), f32),
                pltpu.VMEM((nlon, 8, LANES), f32),
                pltpu.VMEM((16, LANES), f32),
                pltpu.SemaphoreType.DMA((4,)),
                pltpu.SemaphoreType.DMA((16,)),
                pltpu.SemaphoreType.DMA((16,)),
                pltpu.SemaphoreType.DMA((nlat,)),
                pltpu.SemaphoreType.DMA((nlat,)),
                pltpu.SemaphoreType.DMA((nlon,)),
                pltpu.SemaphoreType.DMA((nlon,)),
            ],
            compiler_params=pltpu.CompilerParams(
                collective_id=0, has_side_effects=True, vmem_limit_bytes=32 * 1024 * 1024
            ),
        )(right_side, coefficients, extra, land_mask)

    return jax.shard_map(
        body,
        mesh=mesh,
        in_specs=(P("lat", "lon"), P(None, "lat", "lon"), P("lat", "lon"), P("lat", "lon")),
        out_specs=(P("lat", "lon"), P("lat", "lon"), P()),
        check_vma=False,
    )
```

```python
import functools

import jax
import jax.numpy as jnp
from jax import lax
from jax.experimental import pallas as pl
from jax.experimental.pallas import tpu as pltpu
from jax.sharding import PartitionSpec as P

DEG = 4
ITERS = 3
LOW_EIG = 0.25
HIGH_EIG = 20.5
SHIFT = 0.8
LANES = 128
HALO = 16
VMEM_GRANT = 67043328
STRIP = 16
FIELDS = 7
PAIRS = (FIELDS + 1) // 2
MESH = pl.DeviceIdType.MESH
DIRS = [(a, b) for a in (-1, 0, 1) for b in (-1, 0, 1) if (a, b) != (0, 0)]


def level_factors():
    theta = (HIGH_EIG + LOW_EIG) / 2.0
    delta = (HIGH_EIG - LOW_EIG) / 2.0
    sigma = theta / delta
    rho = 1.0 / sigma
    out = []
    for _ in range(DEG - 1):
        rho_new = 1.0 / (2.0 * sigma - rho)
        out.append((rho_new * rho, 2.0 * rho_new / delta))
        rho = rho_new
    return theta, out


def scalars(h, g):
    c = SHIFT
    ht = [h[k + 1] + c * h[k] for k in range(len(h) - 1)]

    def form(a, t):
        total = None
        for k in range(2 * len(a) - 1):
            pairs = None
            for i in range(len(a)):
                j = k - i
                if 0 <= j < len(a) and i <= j:
                    term = a[i] * a[j]
                    if i != j:
                        term = term + term
                    pairs = term if pairs is None else pairs + term
            pairs = pairs * t[k]
            total = pairs if total is None else total + pairs
        return total

    one = jnp.ones_like(h[0])
    zero = jnp.zeros_like(h[0])
    a = [one]
    b = [one]
    gamma = h[0]
    norms = [g[0]]
    alpha = gamma / ht[0]
    x = [zero] * ITERS
    beta = zero
    for k in range(ITERS):
        if k > 0:
            b = [a[i] + (beta * b[i] if i < len(b) else 0.0) for i in range(len(a))]
        for i in range(len(b)):
            x[i] = x[i] + alpha * b[i]
        tb = [
            (b[i - 1] if i > 0 else zero) + (c * b[i] if i < len(b) else zero)
            for i in range(len(b) + 1)
        ]
        a = [(a[i] if i < len(a) else zero) - alpha * tb[i] for i in range(len(tb))]
        if k < ITERS - 1:
            gamma_new = form(a, h)
            dlt = form(a, ht)
            norms.append(form(a, g))
            beta = gamma_new / gamma
            alpha = gamma_new / (dlt - beta * gamma_new / alpha)
            gamma = gamma_new
    return x, a, norms


def kernel(
    nlat, nlon, rhs_in, coef_in, extra_in, mask_in, x_out, r_out, n_out,
    B, C, E, M, K, V, U, VC, UC, S, Z, SP, RP, SR, RR, G, GL, GZ, T2,
    loc_sem, snd, rcv, lat_s, lat_r, lon_s, lon_r,
):
    rows, cols = rhs_in.shape
    R = rows + 2 * HALO
    W = cols + 2 * LANES
    NC = W // LANES
    ilat = lax.axis_index("lat")
    ilon = lax.axis_index("lon")

    def cs_of(j):
        return slice(j * LANES, (j + 1) * LANES)

    mid = (pl.ds(HALO, rows), pl.ds(LANES, cols))
    local = [
        pltpu.make_async_copy(coef_in, C.at[:, mid[0], mid[1]], loc_sem.at[0]),
        pltpu.make_async_copy(mask_in, M.at[mid[0], mid[1]], loc_sem.at[1]),
        pltpu.make_async_copy(extra_in, E.at[mid[0], mid[1]], loc_sem.at[2]),
        pltpu.make_async_copy(rhs_in, B.at[mid[0], mid[1]], loc_sem.at[3]),
    ]
    for cp in local:
        cp.start()

    def lat_at(d):
        return lax.rem(ilat + d + nlat, nlat)

    def lon_at(d):
        return lax.rem(ilon + d + nlon, nlon)

    barrier = pltpu.get_barrier_semaphore()
    count = 0
    for d in range(1, nlat):
        pl.semaphore_signal(barrier, inc=1, device_id={"lat": lat_at(d)}, device_id_type=MESH)
        count += 1
    for d in range(1, nlon):
        pl.semaphore_signal(barrier, inc=1, device_id={"lon": lon_at(d)}, device_id_type=MESH)
        count += 1
    for a, b in DIRS:
        if a and b:
            pl.semaphore_signal(
                barrier, inc=1, device_id={"lat": lat_at(a), "lon": lon_at(b)}, device_id_type=MESH
            )
            count += 1

    def field(f, rws, cls):
        if f < 4:
            return C[f, rws, cls]
        if f == 4:
            return E[rws, cls]
        if f == 5:
            return B[rws, cls]
        return M[rws, cls].astype(jnp.float32)

    def put(f, rws, cls, value):
        if f < 4:
            C[f, rws, cls] = value
        elif f == 4:
            E[rws, cls] = value
        elif f == 5:
            B[rws, cls] = value
        else:
            M[rws, cls] = value.astype(jnp.int32)

    pl.semaphore_wait(barrier, count)

    sends = []

    def send(src, dst, a, b):
        i = len(sends)
        where = {}
        if a:
            where["lat"] = lat_at(a)
        if b:
            where["lon"] = lon_at(b)
        cp = pltpu.make_async_remote_copy(
            src_ref=src, dst_ref=dst, send_sem=snd.at[i], recv_sem=rcv.at[i],
            device_id=where, device_id_type=MESH,
        )
        cp.start()
        sends.append(cp)

    wide = pl.ds(LANES, cols)
    spans = {
        -1: (pl.ds(HALO, 8), pl.ds(HALO + rows, 8)),
        1: (pl.ds(HALO + rows - 8, 8), pl.ds(HALO - 8, 8)),
    }
    for ref, cp in zip((C, M, E, B), local):
        cp.wait()
        for a, (src, dst) in spans.items():
            if ref is C:
                send(C.at[:, src, wide], C.at[:, dst, wide], a, 0)
            else:
                send(ref.at[src, wide], ref.at[dst, wide], a, 0)

    own_rows = slice(HALO, HALO + rows)
    slot = lax.broadcasted_iota(jnp.int32, (rows, LANES), 1) // STRIP
    for side, chunk in ((0, 1), (1, NC - 2)):
        strip = jnp.zeros((rows, LANES), jnp.float32)
        for f in range(FIELDS):
            turn = (STRIP * f + side * STRIP) % LANES
            a = field(f, own_rows, cs_of(chunk))
            a = pltpu.roll(a, turn, 1) if turn else a
            strip = jnp.where(slot == f, a, strip)
        SP[side] = strip
    upper = lax.broadcasted_iota(jnp.int32, (8, cols), 0) >= 4
    inner = slice(LANES, LANES + cols)
    near = (slice(HALO + 8, HALO + 16), slice(HALO + rows - 16, HALO + rows - 8))
    for side in (0, 1):
        for t in range(PAIRS):
            a = field(2 * t, near[side], inner)
            if 2 * t + 1 < FIELDS:
                b = pltpu.roll(field(2 * t + 1, near[side], inner), 4, 0)
                a = jnp.where(upper, a, b) if side else jnp.where(upper, b, a)
            SR[side, t] = a
    for b in (-1, 1):
        side = (b + 1) // 2
        send(SP.at[side], RP.at[side, pl.ds(HALO, rows)], 0, b)
        for a in (-1, 1):
            src = pl.ds(0, HALO) if a < 0 else pl.ds(rows - HALO, HALO)
            dst = pl.ds(HALO + rows, HALO) if a < 0 else pl.ds(0, HALO)
            send(SP.at[side, src], RP.at[side, dst], a, b)
    for a in (-1, 1):
        side = (a + 1) // 2
        send(SR.at[side], RR.at[side], a, 0)
    for cp in sends:
        cp.wait_recv()

    every = slice(0, R)
    for side, chunk in ((0, NC - 1), (1, 0)):
        strip = RP[side]
        for f in range(FIELDS):
            turn = (-STRIP * f - side * STRIP) % LANES
            put(f, every, cs_of(chunk), pltpu.roll(strip, turn, 1) if turn else strip)
    far = (slice(R - 8, R), slice(0, 8))
    for side in (0, 1):
        for f in range(FIELDS):
            a = RR[side, f // 2]
            put(f, far[side], inner, pltpu.roll(a, 4, 0) if f % 2 else a)

    def shifts(read, n):
        lane = lax.broadcasted_iota(jnp.int32, (n, LANES), 1)
        first = lane == 0
        last = lane == LANES - 1
        memo = {}

        def get(kind, j):
            j = j % NC
            if (kind, j) not in memo:
                if kind == 0:
                    memo[kind, j] = read(j)
                else:
                    memo[kind, j] = pltpu.roll(get(0, j), 1 if kind < 0 else LANES - 1, 1)
            return memo[kind, j]

        def east(j):
            return jnp.where(last, get(1, j + 1), get(1, j))

        def west(j):
            return jnp.where(first, get(-1, j - 1), get(-1, j))

        return (lambda j: get(0, j)), east, west

    def north(a):
        return pltpu.roll(a, a.shape[0] - 1, 0)

    def south(a):
        return pltpu.roll(a, 1, 0)

    grow = lax.broadcasted_iota(jnp.int32, (R, LANES), 0) + (ilat * rows - HALO)
    keep = jnp.where((grow == nlat * rows - 1) | (grow == -1), 0.0, 1.0).astype(jnp.float32)

    mc, mE, mW = shifts(lambda j: M[:, cs_of(j)].astype(jnp.float32), R)
    for j in range(NC):
        m = mc(j)
        me = mE(j)
        mw = mW(j)
        mk = m * keep
        K[1][:, cs_of(j)] = C[0, :, cs_of(j)] * m * me
        K[6][:, cs_of(j)] = C[1, :, cs_of(j)] * mk * north(m)
        K[9][:, cs_of(j)] = C[2, :, cs_of(j)] * mk * north(me)
        K[10][:, cs_of(j)] = C[3, :, cs_of(j)] * mk * north(mw)
        VC[:, cs_of(j)] = B[:, cs_of(j)] * m

    cle, _, wle_of = shifts(lambda j: K[1][:, cs_of(j)], R)
    clne, _, wlne_of = shifts(lambda j: K[9][:, cs_of(j)], R)
    clnw, elnw_of, _ = shifts(lambda j: K[10][:, cs_of(j)], R)
    for j in range(NC):
        le = cle(j)
        wle = wle_of(j)
        ln = K[6][:, cs_of(j)]
        sln = south(ln)
        lne = clne(j)
        wlne = wlne_of(j)
        lnw = clnw(j)
        elnw = elnw_of(j)
        K[2][:, cs_of(j)] = wle
        K[3][:, cs_of(j)] = sln
        K[4][:, cs_of(j)] = south(lne)
        K[5][:, cs_of(j)] = south(lnw)
        K[7][:, cs_of(j)] = wlne
        K[8][:, cs_of(j)] = elnw
        d = E[:, cs_of(j)] + le + wle + ln + sln
        K[0][:, cs_of(j)] = d + lne + south(wlne) + lnw + south(elnw)

    theta, factors = level_factors()

    def apply(ref, rws, finish):
        n = rws.stop - rws.start
        centre, east, west = shifts(lambda j: ref[rws, cs_of(j)], n)
        for j in range(NC):
            v = centre(j)
            ve = east(j)
            vw = west(j)

            def k(i):
                return K[i][rws, cs_of(j)]

            p = k(3) * v + k(4) * ve + k(5) * vw
            q = k(6) * v + k(7) * vw + k(8) * ve
            finish(cs_of(j), v, k(0) * v - k(1) * ve - k(2) * vw - north(p) - south(q))

    mine = slice(HALO, HALO + rows)

    def round_of(it, rws):
        lo = HALO - rws.start

        def level0(cls, v, av):
            z = v * (1.0 / theta)
            step = factors[0][0] * z + factors[0][1] * (v - av * (1.0 / theta))
            S[rws, cls] = step
            Z[0][rws, cls] = z + step

        apply(VC, rws, level0)
        for level in range(1, DEG - 1):
            src = (level - 1) % 2

            def inner_level(cls, z, az):
                qq = VC[rws, cls] - az
                step = factors[level][0] * S[rws, cls] + factors[level][1] * qq
                new = z + step
                if level < DEG - 2:
                    S[rws, cls] = step
                    Z[1 - src][rws, cls] = new
                else:
                    UC[rws, cls] = new
                    U[it, :, cls] = new[lo : lo + rows]

            apply(Z[src], rws, inner_level)

        def last_level(cls, u, au):
            new = au - SHIFT * VC[rws, cls]
            VC[rws, cls] = new
            V[it + 1, :, cls] = new[lo : lo + rows]

        apply(UC, rws, last_level)

    for j in range(1, NC - 1):
        V[0, :, cs_of(j)] = VC[mine, cs_of(j)]
    round_of(0, slice(0, R))

    @pl.loop(1, ITERS)
    def _(it):
        round_of(it, slice(8, R - 8))

    hpairs = [((k + 1) // 2, k // 2) for k in range(2 * ITERS)]
    gpairs = [(k // 2, (k + 1) // 2) for k in range(2 * ITERS - 1)]

    def own(ref, n, j):
        return ref[n, :, cs_of(j)]

    def fold(a):
        return jnp.sum(a.reshape(rows // 8, 8, LANES), axis=0)

    def add(j, acc):
        v = [own(V, n, j) for n in range(ITERS + 1)]
        u = [own(U, n, j) for n in range(ITERS)]
        new = [fold(v[a] * u[b]) for a, b in hpairs] + [fold(v[a] * v[b]) for a, b in gpairs]
        return tuple(p + q for p, q in zip(acc, new))

    nsum = len(hpairs) + len(gpairs)
    acc = tuple(jnp.zeros((8, LANES), jnp.float32) for _ in range(nsum))
    for j in range(1, NC - 1):
        acc = add(j, acc)
    T2[...] = jnp.zeros_like(T2)
    for n, a in enumerate(acc):
        T2[n : n + 1, :] = jnp.sum(a, axis=0, keepdims=True)
    lo = T2[0:8, :]
    hi = T2[8:16, :]
    lo = lo + pltpu.roll(lo, LANES // 2, 1)
    hi = hi + pltpu.roll(hi, LANES // 2, 1)
    half = lax.broadcasted_iota(jnp.int32, (8, LANES), 1) < LANES // 2
    part = jnp.where(half, lo, hi)

    def exchange(part, slot, buf, axis, count, me, at, ssem, rsem):
        G[slot] = part
        buf[me] = part
        cps = []
        for d in range(1, count):
            cp = pltpu.make_async_remote_copy(
                src_ref=G.at[slot],
                dst_ref=buf.at[me],
                send_sem=ssem.at[d],
                recv_sem=rsem.at[d],
                device_id={axis: at(d)},
                device_id_type=MESH,
            )
            cp.start()
            cps.append(cp)
        for cp in cps:
            cp.wait_recv()
        total = buf[0]
        for n in range(1, count):
            total = total + buf[n]
        return total, cps

    total, c1 = exchange(part, 0, GL, "lat", nlat, ilat, lat_at, lat_s, lat_r)
    total, c2 = exchange(total, 1, GZ, "lon", nlon, ilon, lon_at, lon_s, lon_r)

    for n, t in enumerate((jnp.where(half, total, 0.0), jnp.where(half, 0.0, total))):
        s = jnp.sum(t, axis=1, keepdims=True)
        T2[8 * n : 8 * n + 8, :] = jnp.broadcast_to(s, (8, LANES))
    sums = [T2[n : n + 1, :] for n in range(nsum)]
    xs, rs, norms = scalars(sums[: len(hpairs)], sums[len(hpairs) :])

    for j in range(NC - 2):
        x = xs[0] * own(U, 0, j + 1)
        for n in range(1, ITERS):
            x = x + xs[n] * own(U, n, j + 1)
        x_out[:, cs_of(j)] = x
        r = rs[0] * own(V, 0, j + 1)
        for n in range(1, ITERS + 1):
            r = r + rs[n] * own(V, n, j + 1)
        r_out[:, cs_of(j)] = r

    for n in range(ITERS):
        n_out[n] = norms[n][0, 0]
    for cp in sends + c1 + c2:
        cp.wait_send()


def solution(mesh):
    nlat = mesh.shape["lat"]
    nlon = mesh.shape["lon"]

    def body(right_side, coefficients, extra, land_mask):
        rows, cols = right_side.shape
        R, W = rows + 2 * HALO, cols + 2 * LANES
        f32 = jnp.float32
        return pl.pallas_call(
            functools.partial(kernel, nlat, nlon),
            out_shape=(
                jax.ShapeDtypeStruct((rows, cols), f32),
                jax.ShapeDtypeStruct((rows, cols), f32),
                jax.ShapeDtypeStruct((ITERS,), f32),
            ),
            in_specs=[pl.BlockSpec(memory_space=pl.ANY)] * 4,
            out_specs=(
                pl.BlockSpec(memory_space=pltpu.VMEM),
                pl.BlockSpec(memory_space=pltpu.VMEM),
                pl.BlockSpec(memory_space=pltpu.SMEM),
            ),
            scratch_shapes=[
                pltpu.VMEM((R, W), f32),
                pltpu.VMEM((4, R, W), f32),
                pltpu.VMEM((R, W), f32),
                pltpu.VMEM((R, W), jnp.int32),
                [pltpu.VMEM((R, W), f32)] * 11,
                pltpu.VMEM((ITERS + 1, rows, W), f32),
                pltpu.VMEM((ITERS, rows, W), f32),
                pltpu.VMEM((R, W), f32),
                pltpu.VMEM((R, W), f32),
                pltpu.VMEM((R, W), f32),
                [pltpu.VMEM((R, W), f32)] * 2,
                pltpu.VMEM((2, rows, LANES), f32),
                pltpu.VMEM((2, R, LANES), f32),
                pltpu.VMEM((2, PAIRS, 8, cols), f32),
                pltpu.VMEM((2, PAIRS, 8, cols), f32),
                pltpu.VMEM((2, 8, LANES), f32),
                pltpu.VMEM((nlat, 8, LANES), f32),
                pltpu.VMEM((nlon, 8, LANES), f32),
                pltpu.VMEM((16, LANES), f32),
                pltpu.SemaphoreType.DMA((4,)),
                pltpu.SemaphoreType.DMA((16,)),
                pltpu.SemaphoreType.DMA((16,)),
                pltpu.SemaphoreType.DMA((nlat,)),
                pltpu.SemaphoreType.DMA((nlat,)),
                pltpu.SemaphoreType.DMA((nlon,)),
                pltpu.SemaphoreType.DMA((nlon,)),
            ],
            compiler_params=pltpu.CompilerParams(
                collective_id=0, has_side_effects=True, vmem_limit_bytes=VMEM_GRANT
            ),
        )(right_side, coefficients, extra, land_mask)

    return jax.shard_map(
        body,
        mesh=mesh,
        in_specs=(P("lat", "lon"), P(None, "lat", "lon"), P("lat", "lon"), P("lat", "lon")),
        out_specs=(P("lat", "lon"), P("lat", "lon"), P()),
        check_vma=False,
    )
```
